32 devices in a mesh: dp: 4 (over y, core), expert: 8 (over z, x).
Axes of the slice: x: 2, y: 2, z: 4, core: 2. Of those that a mesh axis runs over, the one named last changes fastest.
Arguments:
- tokens: bfloat16 [4096, 1024], P(('dp', 'expert')), may hold values from -6 to 6
- chosen_expert_index: int32 [4096, 6], P(('dp', 'expert')), may hold values from 0 to 7, as said below
- router_gate_weight: float32 [4096, 6], P(('dp', 'expert')), may hold values from 0.05 to 0.5
- output_gradient: bfloat16 [4096, 1024], P(('dp', 'expert')), may hold values from -0.15917969 to 0.15917969
- gate_weight_matrix: bfloat16 [8, 1024, 704], P('expert'), may hold values from -0.1875 to 0.1875
- up_weight: bfloat16 [8, 1024, 704], P('expert'), may hold values from -0.1875 to 0.1875
- down_weight: bfloat16 [8, 704, 1024], P('expert'), may hold values from -0.21875 to 0.21875
- adapter_down_maps: bfloat16 [8, 16, 704], P('expert'), may hold values from -0.21875 to 0.21875
- adapter_up_maps: bfloat16 [8, 16, 1024], P('expert'), may hold values from -1.5 to 1.5
Outputs:
- mixed: bfloat16 [4096, 1024], P(('dp', 'expert'))
- grad_in: bfloat16 [8, 16, 704], P('expert')
- grad_out: bfloat16 [8, 16, 1024], P('expert')
The draws below stay inside these ranges and needn't reach their ends.
Inputs may be any that keep to these rules, and one draw needn't show every extreme that they name: `chosen_expert_index`: each row names 6 different experts. In each aligned block of 128 rows (the rows of one device) no expert is named by more than 126 rows, and one and the same expert, drawn for the whole array, is named by exactly 126 rows of every block. Each row's experts are 6 neighbours in one circular order of all experts, drawn for the whole array.
All inputs are finite; a program needn't handle non-finite values.
Results may differ from the reference program's by a relative error of at most 0.0064.
Values may be sent and summed in bfloat16 or wider, within the bound.
No kernel may reach another device: no remote copies, remote signals or barrier semaphores. Data moves between devices by JAX's collectives and lax.ppermute only.
A program may use at most 64 MiB of HBM per device.

```python
import math
import jax
import jax.numpy as jnp
from jax import lax

MODEL_FEATURES = 1024
HIDDEN_UNITS = 704
ADAPTER_DEPTH = 16
TOPK = 6
TOK_DEV = 128
ROUTED_EXPERTS = 8
TOKENS = 4096
HOT = 21
CAP = 126


def draw_chosen_expert_index(key, part):
    blocks = TOKENS // TOK_DEV
    others = ROUTED_EXPERTS - TOPK
    order_key, spread_keys = jax.random.split(jax.random.fold_in(key, 11))
    labels = jax.random.permutation(order_key, ROUTED_EXPERTS).astype(jnp.int32)
    position = jnp.arange(TOK_DEV, dtype=jnp.int32)
    offsets = jnp.arange(TOPK, dtype=jnp.int32)

    def one_block(block_key):
        shuffle_key, spread_key = jax.random.split(block_key)
        spread = TOPK + jax.random.permutation(spread_key, others).astype(jnp.int32)
        hot_start = position // HOT
        cold_index = jnp.maximum(position - TOPK * HOT, 0) % others
        cold_start = spread[cold_index]
        start_label = jnp.where(position < TOPK * HOT, hot_start, cold_start).astype(jnp.int32)
        start_label = jax.random.permutation(shuffle_key, start_label)
        return labels[(start_label[:, None] + offsets[None, :]) % ROUTED_EXPERTS]
    block_keys = jax.random.split(spread_keys, blocks)
    return jax.vmap(one_block)(block_keys).reshape(TOKENS, TOPK).astype(jnp.int32)


def levels(own_key, dims, cuts, smallest, high):
    def one(axis_at, parts):
        steps = jax.random.uniform(jax.random.fold_in(jax.random.fold_in(own_key, 6), axis_at), (parts,), jnp.float32, smallest / len(cuts), high / len(cuts))
        return jnp.repeat(jnp.exp(steps), dims[axis_at] // parts).reshape((-1,) + (1,) * (len(dims) - axis_at - 1))

    gain = one(*cuts[0])
    for cut in cuts[1:]:
        gain = gain * one(*cut)
    return gain


def scatter_about(own_key, shape, width, bound, cuts=(), held_as=jnp.bfloat16):
    values = width * jax.random.normal(own_key, shape, jnp.float32)
    if cuts:
        values = values * levels(own_key, shape, cuts, -0.22, 0.18)
    return jnp.clip(values, -bound, bound).astype(held_as)


def setup_inputs(seed: int = 0) -> dict:
    seeds = jax.random.split(jax.random.key(seed), 10)
    return {
        "tokens": scatter_about(seeds[0], (TOKENS, MODEL_FEATURES), 1.0, 6.0, ((0, 32),)),
        "chosen_expert_index": draw_chosen_expert_index(jax.random.fold_in(seeds[9], 71), 0),
        "router_gate_weight": jnp.clip(jnp.exp(math.log(0.5) - 2.3025851 * jax.random.uniform(seeds[2], (TOKENS, TOPK), jnp.float32) ** levels(seeds[2], (TOKENS, TOPK), ((0, 32),), -0.2, 0.2)), 0.05, 0.5),
        "output_gradient": scatter_about(seeds[3], (TOKENS, MODEL_FEATURES), 0.02, 0.15917969, ((0, 32),)),
        "gate_weight_matrix": scatter_about(seeds[4], (ROUTED_EXPERTS, MODEL_FEATURES, HIDDEN_UNITS), MODEL_FEATURES ** -0.5, 0.1875, ((0, 8),)),
        "up_weight": scatter_about(seeds[5], (ROUTED_EXPERTS, MODEL_FEATURES, HIDDEN_UNITS), MODEL_FEATURES ** -0.5, 0.1875, ((0, 8),)),
        "down_weight": scatter_about(seeds[6], (ROUTED_EXPERTS, HIDDEN_UNITS, MODEL_FEATURES), HIDDEN_UNITS ** -0.5, 0.21875, ((0, 8),)),
        "adapter_down_maps": scatter_about(seeds[7], (ROUTED_EXPERTS, ADAPTER_DEPTH, HIDDEN_UNITS), HIDDEN_UNITS ** -0.5, 0.21875, ((0, 8),)),
        "adapter_up_maps": scatter_about(seeds[8], (ROUTED_EXPERTS, ADAPTER_DEPTH, MODEL_FEATURES), ADAPTER_DEPTH ** -0.5, 1.5, ((0, 8),)),
    }


def reference(tokens, chosen_expert_index, router_gate_weight, output_gradient, gate_weight_matrix, up_weight, down_weight, adapter_down_maps, adapter_up_maps):
    total_slots = TOKENS * TOPK
    flat_ids = chosen_expert_index.reshape(total_slots).astype(jnp.int32)
    flat_gates = router_gate_weight.reshape(total_slots)
    sort_order = jnp.argsort(flat_ids, stable=True).astype(jnp.int32)
    counts = jnp.bincount(flat_ids, length=ROUTED_EXPERTS).astype(jnp.int32)
    starts = (jnp.cumsum(counts) - counts).astype(jnp.int32)
    bound_rows = (TOKENS // TOK_DEV) * CAP

    def per_expert(running, expert_number):
        position = jnp.arange(bound_rows, dtype=jnp.int32)
        is_live = position < counts[expert_number]
        slot_index = sort_order[jnp.clip(starts[expert_number] + position, 0, total_slots - 1).astype(jnp.int32)]
        token_index = (slot_index // TOPK).astype(jnp.int32)
        slot_gate = jnp.where(is_live, flat_gates[slot_index], jnp.float32(0.0))
        slot_rows = tokens[token_index]
        gate_proj = jnp.dot(slot_rows, gate_weight_matrix[expert_number], preferred_element_type=jnp.float32)
        upward = jnp.dot(slot_rows, up_weight[expert_number], preferred_element_type=jnp.float32)
        hidden_state = (jax.nn.silu(gate_proj) * upward).astype(jnp.bfloat16)
        rank_state = jnp.dot(hidden_state, adapter_down_maps[expert_number].T, preferred_element_type=jnp.float32).astype(jnp.bfloat16)
        slot_out = (jnp.dot(hidden_state, down_weight[expert_number], preferred_element_type=jnp.float32)
                    + jnp.dot(rank_state, adapter_up_maps[expert_number], preferred_element_type=jnp.float32)).astype(jnp.bfloat16)
        running = running.at[token_index].add(slot_gate[:, None] * slot_out.astype(jnp.float32))
        expert_slot_gradient = (slot_gate[:, None] * output_gradient[token_index].astype(jnp.float32)).astype(jnp.bfloat16)
        rank_gradient = jnp.dot(expert_slot_gradient, adapter_up_maps[expert_number].T, preferred_element_type=jnp.float32).astype(jnp.bfloat16)
        grad_hidden = jnp.dot(rank_gradient.T, hidden_state, preferred_element_type=jnp.float32)
        grad_model = jnp.dot(rank_state.T, expert_slot_gradient, preferred_element_type=jnp.float32)
        return running, (grad_hidden, grad_model)

    initial = jnp.zeros((TOKENS, MODEL_FEATURES), jnp.float32)
    mixed_sum, grads = lax.scan(per_expert, initial, jnp.arange(ROUTED_EXPERTS, dtype=jnp.int32))
    return mixed_sum.astype(jnp.bfloat16), grads[0].astype(jnp.bfloat16), grads[1].astype(jnp.bfloat16)
```

```python
import functools

import jax
import jax.numpy as jnp
from jax import lax
from jax.experimental import pallas as pl
from jax.experimental.pallas import tpu as pltpu
from jax.sharding import PartitionSpec as P

BF = jnp.bfloat16
F32 = jnp.float32
VMEM = pltpu.VMEM
SMEM = pltpu.SMEM
NT = (((1,), (1,)), ((), ()))
TN = (((0,), (0,)), ((), ()))


def whole(memory=VMEM):
    return pl.BlockSpec(memory_space=memory)


def call(body, outs, ins, flops, nbytes, scratch=(), smem=0, limit=24, name=None):
    return pl.pallas_call(
        body,
        out_shape=outs,
        in_specs=[whole(SMEM)] * smem + [whole()] * (len(ins) - smem),
        out_specs=jax.tree.map(lambda _: whole(), outs),
        scratch_shapes=list(scratch),
        compiler_params=pltpu.CompilerParams(vmem_limit_bytes=limit * 2**20),
        cost_estimate=pl.CostEstimate(flops=flops, bytes_accessed=nbytes, transcendentals=0),
        name=name,
    )(*ins)


def sds(*shape, dtype=F32):
    return jax.ShapeDtypeStruct(shape, dtype)


def pack_body(experts, tok_ref, idx_ref, gate_ref, out_ref):
    rows, width = tok_ref.shape
    half = rows // 2
    top = idx_ref.shape[1]
    lane = lax.broadcasted_iota(jnp.int32, (rows, 128), 1)
    dense = jnp.zeros((rows, 128), F32)
    for k in range(top):
        dense = dense + jnp.where(lane == idx_ref[:, k : k + 1], gate_ref[:, k : k + 1], 0.0)
    by_expert = dense.T[:experts, :]
    high = by_expert.astype(BF)
    low = (by_expert - high.astype(F32)).astype(BF)
    out_ref[:half, :] = tok_ref[:half, :]
    out_ref[half + experts :, :] = tok_ref[half:, :]
    out_ref[half : half + experts, :] = jnp.zeros((experts, width), BF)
    out_ref[half : half + experts, :rows] = high
    out_ref[half : half + experts, rows : 2 * rows] = low


def spread_gate(block, expert, rows):
    gates = block[:, :rows].astype(F32) + block[:, rows : 2 * rows].astype(F32)
    row = lax.broadcasted_iota(jnp.int32, gates.shape, 0)
    mine = jnp.sum(jnp.where(row == expert, gates, 0.0), axis=0, keepdims=True)
    return jnp.broadcast_to(mine, (128, rows)).T


def scaled(values, gate):
    return values * jnp.concatenate([gate] * (values.shape[1] // 128), axis=1)


def expert_body(kinds, rows, experts, me_ref, *refs):
    count = len(kinds)
    packets = refs[:count]
    gate_w, up_w, down_w, adn, aup = refs[count : count + 5]
    outs = refs[count + 5 : 2 * count + 5]
    hid_ref, lrt_ref, x_ref = refs[2 * count + 5 :]
    half = rows // 2
    me = me_ref[0]
    at = 0
    pieces = []
    for kind, ref in zip(kinds, packets):
        start = at
        if kind in ("full", "top"):
            x_ref[at : at + half, :] = ref[:half, :]
            at += half
        if kind in ("full", "bottom"):
            low = half + experts if kind == "full" else experts
            x_ref[at : at + half, :] = ref[low : low + half, :]
            at += half
        base = 0 if kind == "bottom" else half
        spread = spread_gate(ref[base : base + experts, :], me, rows)
        if kind == "top":
            spread = spread[:half, :]
        if kind == "bottom":
            spread = spread[half:, :]
        pieces.append((start, at, spread))
    x = x_ref[...]
    gate_proj = jnp.dot(x, gate_w[...], preferred_element_type=F32)
    upward = jnp.dot(x, up_w[...], preferred_element_type=F32)
    hid = (gate_proj / (1.0 + jnp.exp(-gate_proj)) * upward).astype(BF)
    hid_ref[...] = hid
    lrt = lax.dot_general(adn[...], hid, NT, preferred_element_type=F32).astype(BF)
    lrt_ref[...] = lrt
    out = jnp.dot(hid, down_w[...], preferred_element_type=F32) + lax.dot_general(
        lrt, aup[...], TN, preferred_element_type=F32
    )
    out = out.astype(BF).astype(F32)
    for (start, stop, spread), ref in zip(pieces, outs):
        ref[...] = scaled(out[start:stop, :], spread).astype(ref.dtype)


def expert(me, packets, kinds, rows, experts, weights):
    gate_w, up_w, down_w, adn, aup = weights
    width, hidden = gate_w.shape
    depth = adn.shape[0]
    sizes = [rows if kind == "full" else rows // 2 for kind in kinds]
    total = sum(sizes)
    outs = [sds(size, width) for size in sizes]
    outs += [sds(total, hidden, dtype=BF), sds(depth, total, dtype=BF)]
    result = call(
        functools.partial(expert_body, kinds, rows, experts),
        outs,
        [me, *packets, *weights],
        6 * total * width * hidden,
        6 * width * hidden + 8 * total * width,
        scratch=[pltpu.VMEM((total, width), BF)],
        smem=1,
        limit=24,
        name="expert",
    )
    return result[: len(kinds)], result[-2], result[-1]


def helper_pieces(side, last, half):
    rows = 2 * half
    if side > 0:
        third = (0, 0, half) if last else (0, 0, rows)
        return ((2, 0, rows), (1, 0, rows), third)
    third = (2, half, rows) if last else (2, 0, rows)
    return ((0, 0, rows), (1, 0, rows), third)


def first_grad_body(jobs, rows, experts, ids_ref, *refs):
    half = rows // 2
    grads, packets, lrts, hids, (aup,) = refs[:3], refs[3:6], refs[6:9], refs[9:12], refs[12:13]
    aups = refs[13 : 13 + len(jobs)]
    gin_ref, gout_ref = refs[13 + len(jobs) : 15 + len(jobs)]
    lgt_refs = refs[15 + len(jobs) :]
    blocks = [ref[half : half + experts, :] for ref in packets]
    values = [ref[...].astype(F32) for ref in grads]
    gin = gout = None
    for block, value, lrt, hid in zip(blocks, values, lrts, hids):
        slot = scaled(value, spread_gate(block, ids_ref[0], rows)).astype(BF)
        lgt = lax.dot_general(aup[...], slot, NT, preferred_element_type=F32).astype(BF)
        one = jnp.dot(lgt, hid[...], preferred_element_type=F32)
        two = jnp.dot(lrt[...], slot, preferred_element_type=F32)
        gin = one if gin is None else gin + one
        gout = two if gout is None else gout + two
    gin_ref[...] = gin
    gout_ref[...] = gout
    for at, (side, last) in enumerate(jobs):
        lgt_refs[at][...] = jnp.zeros(lgt_refs[at].shape, BF)
        spot = 0
        for source, low, high in helper_pieces(side, last, half):
            spread = spread_gate(blocks[source], ids_ref[1 + at], rows)
            slot = scaled(values[source][low:high, :], spread[low:high, :]).astype(BF)
            lgt_refs[at][:, spot : spot + high - low] = lax.dot_general(
                aups[at][...], slot, NT, preferred_element_type=F32
            ).astype(BF)
            spot += high - low


def second_grad_body(jobs, rows, experts, ids_ref, *refs):
    half = rows // 2
    depth = refs[6].shape[0]
    grads, packets, gin0 = refs[:3], refs[3:6], refs[6]
    count = len(jobs)
    recv = refs[7 : 7 + count]
    hids = refs[7 + count : 7 + 2 * count]
    gin_ref = refs[7 + 2 * count]
    helped = refs[8 + 2 * count :]
    blocks = [ref[half : half + experts, :] for ref in packets]
    gin = gin0[...]
    for at, (side, last) in enumerate(jobs):
        spot = 0
        total = None
        for source, low, high in helper_pieces(side, last, half):
            spread = spread_gate(blocks[source], ids_ref[1 + at], rows)
            value = grads[source][low:high, :].astype(F32)
            slot = scaled(value, spread[low:high, :]).astype(BF)
            part = jnp.dot(
                recv[at][:depth, spot : spot + high - low], slot, preferred_element_type=F32
            )
            total = part if total is None else total + part
            spot += high - low
        helped[at][...] = total
        gin = gin + jnp.dot(
            recv[at][depth:, :spot], hids[at][...], preferred_element_type=F32
        )
    gin_ref[...] = gin


def shards(
    tokens,
    chosen_expert_index,
    router_gate_weight,
    output_gradient,
    gate_weight_matrix,
    up_weight,
    down_weight,
    adapter_down_maps,
    adapter_up_maps,
):
    rows, width = tokens.shape
    half = rows // 2
    hidden = gate_weight_matrix.shape[2]
    depth = adapter_down_maps.shape[1]
    ring = lax.axis_size("expert")
    replicas = lax.axis_size("dp")
    experts = ring * gate_weight_matrix.shape[0]
    far = ring // 2
    order = list(range(0, ring, 2)) + list(range(ring - 1, 0, -2))
    place = {device: spot for spot, device in enumerate(order)}

    def hop(value, by):
        pairs = [(order[spot], order[(spot + by) % ring]) for spot in range(ring)]
        return lax.ppermute(value, "expert", pairs)

    me = lax.axis_index("expert").astype(jnp.int32)
    order_table = jnp.array(order, jnp.int32)
    spot = jnp.array([place[device] for device in range(ring)], jnp.int32)[me]

    def at_offset(by):
        return order_table[(spot + by) % ring]

    weights = (
        gate_weight_matrix[0],
        up_weight[0],
        down_weight[0],
        adapter_down_maps[0],
        adapter_up_maps[0],
    )
    aup = weights[4]
    me1 = me.reshape(1)

    own = call(
        functools.partial(pack_body, experts),
        sds(rows + experts, width, dtype=BF),
        [tokens, chosen_expert_index, router_gate_weight],
        rows * width,
        4 * rows * width,
        name="pack",
    )

    left, right = {0: own}, {0: own}
    for step in range(1, far):
        left[step] = hop(left[step - 1], 1)
        right[step] = hop(right[step - 1], -1)
    left[far] = hop(left[far - 1][: half + experts], 1)
    right[far] = hop(right[far - 1][half:], -1)
    og = (hop(output_gradient, 1), output_gradient, hop(output_gradient, -1))

    reach = [(3 * j, 3 * j + 1 == far) for j in range(1, (far - 1) // 3 + 1)]
    jobs = tuple((side, last) for _, last in reach for side in (1, -1))
    shifts = [side * by for by, _ in reach for side in (1, -1)]
    aups = [hop(aup, -shift) for shift in shifts]

    run = functools.partial(expert, me1, rows=rows, experts=experts, weights=weights)
    share, hid, lrt = {}, {}, {}
    (share[0],), hid[0], lrt[0] = run([own], ("full",))
    for step in range(1, far):
        (a, b), h, low = run([left[step], right[step]], ("full", "full"))
        share[-step], share[step] = a, b
        hid[-step], hid[step] = h[:rows], h[rows:]
        lrt[-step], lrt[step] = low[:, :rows], low[:, rows:]
    (far_top, far_bottom), far_hid, far_lrt = run([left[far], right[far]], ("top", "bottom"))

    def add(value, mine):
        return (value.astype(F32) + mine).astype(BF)

    def chain(first, way, piece):
        value = first
        for step in range(far - 1, 0, -1):
            mine = share[way * step][piece]
            value = mine.astype(BF) if value is None else add(value, mine)
            value = hop(value, way)
        return value

    top, bottom = slice(0, half), slice(half, rows)
    a_top = chain(hop(far_top.astype(BF), 1), 1, top)
    b_bottom = chain(hop(far_bottom.astype(BF), -1), -1, bottom)
    a_bottom = chain(None, 1, bottom)
    b_top = chain(None, -1, top)
    mixed_top = (a_top.astype(F32) + b_top.astype(F32) + share[0][top]).astype(BF)
    mixed_bottom = (a_bottom.astype(F32) + b_bottom.astype(F32) + share[0][bottom]).astype(BF)
    mixed = jnp.concatenate([mixed_top, mixed_bottom])

    ids = jnp.stack([me] + [at_offset(shift) for shift in shifts])
    window = (left[1], own, right[1])
    wide = 3 * rows
    first = call(
        functools.partial(first_grad_body, jobs, rows, experts),
        [sds(depth, hidden), sds(depth, width)] + [sds(depth, wide, dtype=BF) for _ in jobs],
        [
            ids,
            *og,
            *window,
            lrt[-1],
            lrt[0],
            lrt[1],
            hid[-1],
            hid[0],
            hid[1],
            aup,
            *aups,
        ],
        10 * rows * width * depth,
        10 * rows * width,
        smem=1,
        name="first_grad",
    )
    gin, gout, lgts = first[0], first[1], first[2:]

    def beyond(table, by, side, last, far_value, axis):
        pieces = [table[side * (by - 1)], table[side * by]]
        if last:
            pieces.append(far_value)
        else:
            pieces.append(table[side * (by + 1)])
        return jnp.concatenate(pieces, axis=axis)

    recv, beyond_hid = [None] * len(jobs), []
    for at, ((side, last), shift) in enumerate(zip(jobs, shifts)):
        by = abs(shift)
        far_l = far_lrt[:, half:] if side > 0 else far_lrt[:, :half]
        far_h = far_hid[half:] if side > 0 else far_hid[:half]
        rank = beyond(lrt, by, side, last, far_l, 1)
        rank = jnp.pad(rank, ((0, 0), (0, wide - rank.shape[1])))
        sent = hop(jnp.concatenate([rank, lgts[at]], axis=0), shift)
        recv[at ^ 1] = sent
        beyond_hid.append(beyond(hid, by, side, last, far_h, 0))
    second = call(
        functools.partial(second_grad_body, jobs, rows, experts),
        [sds(depth, hidden)] + [sds(depth, width) for _ in jobs],
        [ids, *og, *window, gin, *recv, *beyond_hid],
        10 * rows * width * depth,
        10 * rows * width,
        smem=1,
        name="second_grad",
    )
    gin = second[0]
    for shift, part in zip(shifts, second[1:]):
        gout = gout + hop(part, shift)
    both = jnp.concatenate([gin, gout], axis=1)
    by = 1
    while by < replicas:
        both = both + lax.ppermute(both, "dp", [(i, i ^ by) for i in range(replicas)])
        by *= 2
    grads = both.astype(BF)
    return mixed, grads[None, :, :hidden], grads[None, :, hidden:]


def solution(mesh):
    rows = P(("dp", "expert"), None)
    held = P("expert", None, None)
    return jax.shard_map(
        shards,
        mesh=mesh,
        in_specs=(rows, rows, rows, rows, held, held, held, held, held),
        out_specs=(rows, held, held),
        check_vma=False,
    )
```
